32 devices in a mesh: floor: 4 (over y, x), zone: 8 (over z, core).
Axes of the slice: x: 2, y: 2, z: 4, core: 2. Of those that a mesh axis runs over, the one named last changes fastest.
Arguments:
- factor: float32 [512, 96, 384], P(('floor', 'zone')), may hold values from -0.625 to 0.625
- plant_map: float32 [512, 96, 384], P(('floor', 'zone')), may hold values from -0.4082483 to 0.4082483
- offset: float32 [512, 384], P(('floor', 'zone')), may hold values from -10 to 10
- start_plan: float32 [512, 384], P(('floor', 'zone')), may hold values from -10 to 10
- demand: float32 [4, 48], replicated, may hold values from -768 to 768
- start_price: float32 [4, 48], replicated, may hold values from -6 to 6
- start_multiplier: float32 [512, 48], P(('floor', 'zone')), may hold values from -6 to 6
- neighbors: int32 [512, 4], P(('floor', 'zone')), may hold values from 0 to 127
- loop_of_zone: int32 [512], P(('floor', 'zone')), may hold values from 0 to 3
Outputs:
- control: float32 [512, 384], P(('floor', 'zone'))
- price: float32 [4, 48], replicated
- multiplier: float32 [512, 48], P(('floor', 'zone'))
The draws below stay inside these ranges and needn't reach their ends.
Inputs may be any that keep to these rules, and one draw needn't show every extreme that they name: `neighbors`: indices count zones within the zone's own floor of 128 consecutive zones.
All inputs are finite; a program needn't handle non-finite values.
Results may differ from the reference program's by a relative error of at most 0.0001.
Values sent between devices are 32-bit elements; how exact they have to be, the bound alone decides.
No kernel may reach another device: no remote copies, remote signals or barrier semaphores. Data moves between devices by JAX's collectives and lax.ppermute only.
A program may use at most 64 MiB of HBM per device.

```python
import math
import jax
import jax.numpy as jnp
from jax import lax

HORIZON = 48
NEIGHBORS = 4
LOOPS = 4
ITERS = 2
CONTROLS = 384
FLOOR_ZONES = 128
ZONES = 512


def common_parts(key):
    base = jax.random.fold_in(key, 5171)
    key_map, key_plan = jax.random.split(base)
    map_scale = 1.0 / math.sqrt(CONTROLS)
    shared_map = jnp.clip(jax.random.normal(key_map, (HORIZON, CONTROLS), jnp.float32), -4.0, 4.0) * map_scale
    shared_plan = jnp.clip(jax.random.normal(key_plan, (CONTROLS,), jnp.float32), -4.0, 4.0)
    return (shared_map, shared_plan)


def zone_noise(key, shape):
    return jnp.clip(jax.random.normal(key, shape, jnp.float32), -4.0, 4.0)


def draw_plant_map(key, part):
    shared_map, shared_plan = common_parts(key)
    own_key = jax.random.fold_in(key, 5172)
    map_scale = 1.0 / math.sqrt(CONTROLS)
    noise = zone_noise(own_key, (ZONES, 2 * HORIZON, CONTROLS)) * map_scale
    head = noise[:, :HORIZON, :] + shared_map[None, :, :]
    return jnp.concatenate([head, noise[:, HORIZON:, :]], axis=1).astype(jnp.float32)


def draw_start_plan(key, part):
    shared_map, shared_plan = common_parts(key)
    own_key = jax.random.fold_in(key, 5173)
    noise = zone_noise(own_key, (ZONES, CONTROLS))
    return (shared_plan[None, :] + noise).astype(jnp.float32)


def draw_offset(key, part):
    shared_map, shared_plan = common_parts(key)
    own_key = jax.random.fold_in(key, 5174)
    noise = zone_noise(own_key, (ZONES, CONTROLS))
    return (noise - shared_plan[None, :]).astype(jnp.float32)


def plant(values, key, least, top_value):
    dims = values.shape
    index_at = [jax.random.randint(jax.random.fold_in(key, axis), (), 0, dims[axis]) for axis in range(len(dims))]
    values = values.at[tuple(index_at)].set(least)
    longest = dims.index(max(dims))
    index_at[longest] = (index_at[longest] + 1) % dims[longest]
    return values.at[tuple(index_at)].set(top_value)


def block_scale(key, dims, cuts, smallest, largest):
    factor_of = 1.0
    for position, shards_of in cuts:
        draws = jax.random.uniform(jax.random.fold_in(jax.random.fold_in(key, 6), position), (shards_of,), jnp.float32, smallest / len(cuts), largest / len(cuts))
        factor_of = factor_of * jnp.repeat(jnp.exp(draws), dims[position] // shards_of).reshape((-1,) + (1,) * (len(dims) - 1 - position))
    return factor_of


def bell_draw(key, shape, width, limit, shards=(), kind=jnp.bfloat16):
    drawn = width * jax.random.normal(key, shape, jnp.float32)
    if shards:
        drawn = drawn * block_scale(key, shape, shards, -0.22, 0.18)
    return jnp.clip(drawn, -limit, limit).astype(kind)


def setup_inputs(seed: int = 0) -> dict:
    splits = jax.random.split(jax.random.key(seed), 10)
    return {
        "factor": bell_draw(splits[0], (ZONES, 2 * HORIZON, CONTROLS), (2 * HORIZON) ** -0.5, 0.625, ((0, 32),), jnp.float32),
        "plant_map": draw_plant_map(jax.random.fold_in(splits[9], 71), 0),
        "offset": draw_offset(jax.random.fold_in(splits[9], 71), 0),
        "start_plan": draw_start_plan(jax.random.fold_in(splits[9], 71), 0),
        "demand": bell_draw(splits[4], (LOOPS, HORIZON), (ZONES // LOOPS), 768.0, (), jnp.float32),
        "start_price": bell_draw(splits[5], (LOOPS, HORIZON), 1.0, 6.0, (), jnp.float32),
        "start_multiplier": bell_draw(splits[6], (ZONES, HORIZON), 1.0, 6.0, ((0, 32),), jnp.float32),
        "neighbors": plant(jax.random.randint(splits[7], (ZONES, NEIGHBORS), 0, FLOOR_ZONES), jax.random.fold_in(splits[7], 1), 0, FLOOR_ZONES - 1).astype(jnp.int32),
        "loop_of_zone": plant(jax.random.randint(splits[8], (ZONES,), 0, LOOPS), jax.random.fold_in(splits[8], 1), 0, LOOPS - 1).astype(jnp.int32),
    }


def reference(factor, plant_map, offset, start_plan, demand, start_price, start_multiplier, neighbors, loop_of_zone):
    control = start_plan
    price = start_price
    multiplier = start_multiplier
    onehot = (loop_of_zone[:, None] == jnp.arange(LOOPS, dtype=jnp.int32)[None, :]).astype(jnp.float32)
    floor_base = (jnp.arange(ZONES, dtype=jnp.int32) // FLOOR_ZONES) * FLOOR_ZONES
    global_index = (floor_base[:, None] + neighbors).astype(jnp.int32)
    for step in range(ITERS):
        outputs = jnp.einsum("zkv,zv->zk", plant_map, control, precision=lax.Precision.HIGHEST)
        shares = outputs[:, :HORIZON]
        bound = outputs[:, HORIZON:]
        total = jnp.dot(onehot.T, shares, precision=lax.Precision.HIGHEST)
        excess = (total - demand) * (LOOPS / ZONES)
        shift = jnp.dot(onehot, excess + price, precision=lax.Precision.HIGHEST)
        price = price + excess
        target_share = shares - shift
        near = jnp.mean(bound[global_index], axis=1)
        target_bound = (bound + near) / 2.0 - multiplier
        multiplier = multiplier + (bound - near) / 2.0
        target = jnp.concatenate([target_share, target_bound], axis=1)
        control = 0.8 * jnp.einsum("zkv,zk->zv", factor, target, precision=lax.Precision.HIGHEST) - offset
    return control, price, multiplier
```

```python
import jax
import jax.numpy as jnp
from jax import lax
from jax.sharding import PartitionSpec as P

HORIZON = 48
NEIGHBORS = 4
LOOPS = 4
ITERS = 2


def select_rows(neighbors, count):
    columns = jnp.arange(count, dtype=jnp.int32)
    picks = (neighbors[:, :, None] == columns[None, None, :]).astype(jnp.float32)
    return jnp.sum(picks, axis=1) / NEIGHBORS


def local(
    factor,
    plant_map,
    offset,
    start_plan,
    demand,
    start_price,
    start_multiplier,
    neighbors,
    loop_of_zone,
):
    control = start_plan
    price = start_price
    multiplier = start_multiplier
    zones_here = control.shape[0]
    per_floor = lax.axis_size("zone")
    devices = lax.axis_size("floor") * per_floor
    floor = lax.axis_index("floor")
    zones_all = zones_here * devices
    onehot = (loop_of_zone[:, None] == jnp.arange(LOOPS, dtype=jnp.int32)[None, :]).astype(
        jnp.float32
    )
    for step in range(ITERS):
        outputs = jnp.einsum("zkv,zv->zk", plant_map, control, precision=lax.Precision.HIGHEST)
        shares = outputs[:, :HORIZON]
        bound = outputs[:, HORIZON:]
        partial_load = jnp.dot(onehot.T, shares, precision=lax.Precision.HIGHEST)
        packed = jnp.concatenate([bound, partial_load], axis=0)
        spread = jnp.broadcast_to(packed[None], (devices,) + packed.shape)
        got = lax.all_to_all(spread, ("floor", "zone"), 0, 0)
        total = jnp.sum(got[:, zones_here:], axis=0)
        excess = (total - demand) * (LOOPS / zones_all)
        shift = jnp.dot(onehot, excess + price, precision=lax.Precision.HIGHEST)
        price = price + excess
        target_share = shares - shift
        own_floor = lax.dynamic_slice_in_dim(got, floor * per_floor, per_floor, 0)
        floor_bound = own_floor[:, :zones_here].reshape(per_floor * zones_here, HORIZON)
        weights = select_rows(neighbors, floor_bound.shape[0])
        near = jnp.dot(weights, floor_bound, precision=lax.Precision.HIGHEST)
        target_bound = (bound + near) / 2.0 - multiplier
        multiplier = multiplier + (bound - near) / 2.0
        target = jnp.concatenate([target_share, target_bound], axis=1)
        control = (
            0.8 * jnp.einsum("zkv,zk->zv", factor, target, precision=lax.Precision.HIGHEST) - offset
        )
    return (control, price, multiplier)


def solution(mesh):
    placed = (
        P(("floor", "zone"), None, None),
        P(("floor", "zone"), None, None),
        P(("floor", "zone"), None),
        P(("floor", "zone"), None),
        P(),
        P(),
        P(("floor", "zone"), None),
        P(("floor", "zone"), None),
        P(("floor", "zone")),
    )
    return jax.shard_map(
        local,
        mesh=mesh,
        in_specs=placed,
        out_specs=(P(("floor", "zone"), None), P(), P(("floor", "zone"), None)),
        check_vma=False,
    )
```

```python
import functools

import jax
import jax.numpy as jnp
from jax import lax
from jax.experimental import pallas as pl
from jax.experimental.pallas import tpu as pltpu
from jax.sharding import PartitionSpec as P

LOOPS = 4
ITERS = 2
LANES = 128
EXACT = lax.Precision.HIGHEST


def iota(shape, dim):
    return lax.broadcasted_iota(jnp.int32, shape, dim)


def dot(a, b):
    return jnp.dot(a, b, precision=EXACT, preferred_element_type=jnp.float32)


def dot_rows(a, b):
    return lax.dot_general(
        a, b, (((0,), (0,)), ((), ())), precision=EXACT, preferred_element_type=jnp.float32
    )


def members(loop, rows):
    return (iota((rows, loop.shape[1]), 0) == loop).astype(jnp.float32)


def outputs_of(maps, control, zones, wide):
    lane = iota((wide, LANES), 1)
    columns = jnp.zeros((wide, LANES), jnp.float32)
    controls = control.shape[1]
    for z in range(zones):
        row = control[z : z + 1]
        block = maps(z)
        part = block[:, :LANES] * row[:, :LANES]
        for v in range(LANES, controls, LANES):
            part = part + block[:, v : v + LANES] * row[:, v : v + LANES]
        columns = jnp.where(lane == z, jnp.sum(part, axis=1, keepdims=True), columns)
    square = jnp.concatenate([columns, jnp.zeros((LANES - wide, LANES), jnp.float32)], axis=0)
    return square.T[:zones]


def decide(factor, target, zones, wide):
    square = jnp.concatenate([target, jnp.zeros((LANES - zones, LANES), jnp.float32)], axis=0)
    columns = square.T[:wide]
    rows = []
    for z in range(zones):
        rows.append(jnp.sum(factor(z) * columns[:, z : z + 1], axis=0, keepdims=True))
    return 0.8 * jnp.concatenate(rows, axis=0)


def pack(out, loop, horizon, zones):
    half = zones // 2
    loads = dot(members(loop, half), out)
    lane = iota((half, LANES), 1)
    row = iota((half, LANES), 0)
    first = pltpu.roll(out[:half], LANES - horizon, 1)
    rest = LANES - 2 * horizon
    ahead = pltpu.roll(loads, 2 * horizon, 1)
    behind = pltpu.roll(pltpu.roll(loads, 2 * horizon - rest, 1), LOOPS, 0)
    block = jnp.where(lane < horizon, first, out[half:])
    return jnp.where(lane < 2 * horizon, block, jnp.where(row < LOOPS, ahead, behind))


def total_of(got_ref, horizon):
    total = jnp.sum(got_ref[...], axis=0)
    rest = LANES - 2 * horizon
    lane = iota(total.shape, 1)
    ahead = pltpu.roll(total, LANES - 2 * horizon, 1)
    behind = pltpu.roll(pltpu.roll(total, LANES - 2 * horizon + rest, 1), total.shape[0] - LOOPS, 0)
    return jnp.where(lane < rest, ahead, behind)


def near_of(got_ref, neighbors, per_floor, horizon, zones):
    half = zones // 2
    own = got_ref[pl.ds(lax.axis_index("floor") * per_floor, per_floor)].reshape(per_floor * half, LANES)
    column = iota((per_floor * half, zones), 0)
    low = (column // half) * zones + column % half
    count = neighbors.shape[0]
    pick_low = jnp.zeros(column.shape, jnp.float32)
    pick_high = pick_low
    for b in range(count):
        which = neighbors[b : b + 1]
        pick_low = pick_low + (which == low).astype(jnp.float32)
        pick_high = pick_high + (which == low + half).astype(jnp.float32)
    return (pltpu.roll(dot_rows(pick_low, own), horizon, 1) + dot_rows(pick_high, own)) / count


def widen(ref, scratch, shift):
    scratch[...] = jnp.zeros_like(scratch)
    scratch[: ref.shape[0], : ref.shape[1]] = ref[...]
    value = scratch[...]
    return pltpu.roll(value, shift, 1) if shift else value


def consensus(got_ref, out, price, multiplier, demand, neighbors, loop, per_floor, scale, horizon):
    zones = out.shape[0]
    lane = iota((zones, LANES), 1)
    excess = (total_of(got_ref, horizon) - demand) * scale
    shift = dot_rows(members(loop, price.shape[0]), excess + price)
    near = near_of(got_ref, neighbors, per_floor, horizon, zones)
    target = jnp.where(lane < horizon, out - shift, (out + near) / 2.0 - multiplier)
    return target, price + excess, multiplier + (out - near) / 2.0


def first_kernel(horizon, map_ref, plan_ref, loop_ref, out_ref, send_ref):
    zones, wide = map_ref.shape[0], map_ref.shape[1]
    out = outputs_of(lambda z: map_ref[z], plan_ref[...], zones, wide)
    out_ref[...] = out
    block = pack(out, loop_ref[...], horizon, zones)
    send_ref[...] = jnp.broadcast_to(block[None], send_ref.shape)


def middle_kernel(
    per_floor, scale, horizon,
    got_ref, out_ref, price_ref, mult_ref, demand_ref, nb_ref, loop_ref,
    offset_ref, factor_ref, map_ref,
    next_out_ref, next_price_ref, next_mult_ref, send_ref, wide8, wide16,
):
    zones, wide = map_ref.shape[0], map_ref.shape[1]
    target, price, mult = consensus(
        got_ref, out_ref[...], widen(price_ref, wide8, 0), widen(mult_ref, wide16, horizon),
        widen(demand_ref, wide8, 0), nb_ref[...], loop_ref[...], per_floor, scale, horizon,
    )
    next_price_ref[...] = price
    next_mult_ref[...] = mult
    control = decide(lambda z: factor_ref[z], target, zones, wide) - offset_ref[...]
    out = outputs_of(lambda z: map_ref[z], control, zones, wide)
    next_out_ref[...] = out
    block = pack(out, loop_ref[...], horizon, zones)
    send_ref[...] = jnp.broadcast_to(block[None], send_ref.shape)


def last_kernel(
    per_floor, scale, horizon,
    got_ref, out_ref, price_ref, mult_ref, demand_ref, nb_ref, loop_ref, offset_ref, factor_ref,
    control_ref, next_price_ref, next_mult_ref, wide8,
):
    zones, wide = factor_ref.shape[0], factor_ref.shape[1]
    target, price, mult = consensus(
        got_ref, out_ref[...], price_ref[...], mult_ref[...], widen(demand_ref, wide8, 0),
        nb_ref[...], loop_ref[...], per_floor, scale, horizon,
    )
    next_price_ref[...] = price[: next_price_ref.shape[0], :horizon]
    next_mult_ref[...] = pltpu.roll(mult, LANES - horizon, 1)[:, :horizon]
    control_ref[...] = decide(lambda z: factor_ref[z], target, zones, wide) - offset_ref[...]


def local(
    factor, plant_map, offset, start_plan, demand, start_price, start_multiplier, neighbors, loop_of_zone
):
    zones, wide, controls = plant_map.shape
    horizon = wide // 2
    half = zones // 2
    per_floor = lax.axis_size("zone")
    devices = lax.axis_size("floor") * per_floor
    scale = LOOPS / (zones * devices)
    loop_row = loop_of_zone[None, :]
    neighbors = neighbors.T
    vmem = pl.BlockSpec(memory_space=pltpu.VMEM)
    f32 = jnp.float32
    rows = jax.ShapeDtypeStruct((zones, LANES), f32)
    send = jax.ShapeDtypeStruct((devices, half, LANES), f32)
    eight = jax.ShapeDtypeStruct((half, LANES), f32)
    params = pltpu.CompilerParams(vmem_limit_bytes=24 * 1024 * 1024)

    out, spread = pl.pallas_call(
        functools.partial(first_kernel, horizon),
        out_shape=(rows, send),
        in_specs=[vmem] * 3,
        out_specs=(vmem, vmem),
        compiler_params=params,
        name="first",
    )(plant_map, start_plan, loop_row)
    price, multiplier = start_price, start_multiplier
    for step in range(ITERS - 1):
        got = lax.all_to_all(spread, ("floor", "zone"), 0, 0)
        out, price, multiplier, spread = pl.pallas_call(
            functools.partial(middle_kernel, per_floor, scale, horizon),
            out_shape=(rows, eight, rows, send),
            in_specs=[vmem] * 10,
            out_specs=(vmem,) * 4,
            scratch_shapes=[pltpu.VMEM((half, LANES), f32), pltpu.VMEM((zones, LANES), f32)],
            compiler_params=params,
            name="middle",
        )(
            got, out, price, multiplier, demand, neighbors, loop_row,
            offset, factor, plant_map,
        )
    got = lax.all_to_all(spread, ("floor", "zone"), 0, 0)
    return pl.pallas_call(
        functools.partial(last_kernel, per_floor, scale, horizon),
        out_shape=(
            jax.ShapeDtypeStruct((zones, controls), f32),
            jax.ShapeDtypeStruct(start_price.shape, f32),
            jax.ShapeDtypeStruct(start_multiplier.shape, f32),
        ),
        in_specs=[vmem] * 9,
        out_specs=(vmem,) * 3,
        scratch_shapes=[pltpu.VMEM((half, LANES), f32)],
        compiler_params=params,
        name="last",
    )(got, out, price, multiplier, demand, neighbors, loop_row, offset, factor)


def solution(mesh):
    placed = (
        P(("floor", "zone"), None, None),
        P(("floor", "zone"), None, None),
        P(("floor", "zone"), None),
        P(("floor", "zone"), None),
        P(),
        P(),
        P(("floor", "zone"), None),
        P(("floor", "zone"), None),
        P(("floor", "zone")),
    )
    return jax.shard_map(
        local,
        mesh=mesh,
        in_specs=placed,
        out_specs=(P(("floor", "zone"), None), P(), P(("floor", "zone"), None)),
        check_vma=False,
    )
```

```python
import functools

import jax
import jax.numpy as jnp
from jax import lax
from jax.experimental import pallas as pl
from jax.experimental.pallas import tpu as pltpu
from jax.sharding import PartitionSpec as P

LOOPS = 4
ITERS = 2
LANES = 128
EXACT = lax.Precision.HIGHEST


def iota(shape, dim):
    return lax.broadcasted_iota(jnp.int32, shape, dim)


def dot(a, b):
    return jnp.dot(a, b, precision=EXACT, preferred_element_type=jnp.float32)


def dot_rows(a, b):
    return lax.dot_general(
        a, b, (((0,), (0,)), ((), ())), precision=EXACT, preferred_element_type=jnp.float32
    )


def members(loop, rows):
    return (iota((rows, loop.shape[1]), 0) == loop).astype(jnp.float32)


def outputs_of(maps, control, zones, wide):
    lane = iota((wide, LANES), 1)
    columns = jnp.zeros((wide, LANES), jnp.float32)
    controls = control.shape[1]
    for z in range(zones):
        row = control[z : z + 1]
        block = maps(z)
        part = block[:, :LANES] * row[:, :LANES]
        for v in range(LANES, controls, LANES):
            part = part + block[:, v : v + LANES] * row[:, v : v + LANES]
        columns = jnp.where(lane == z, jnp.sum(part, axis=1, keepdims=True), columns)
    square = jnp.concatenate([columns, jnp.zeros((LANES - wide, LANES), jnp.float32)], axis=0)
    return square.T[:zones]


def decide(factor, target, zones, wide):
    square = jnp.concatenate([target, jnp.zeros((LANES - zones, LANES), jnp.float32)], axis=0)
    columns = square.T[:wide]
    rows = []
    for z in range(zones):
        rows.append(jnp.sum(factor(z) * columns[:, z : z + 1], axis=0, keepdims=True))
    return 0.8 * jnp.concatenate(rows, axis=0)


def pack(out, loop, rows, horizon, zones):
    half = zones // 2
    loads = dot((rows[:, :zones] == loop).astype(jnp.float32), out)
    lane = iota((half, LANES), 1)
    row = iota((half, LANES), 0)
    first = pltpu.roll(out[:half], LANES - horizon, 1)
    rest = LANES - 2 * horizon
    ahead = pltpu.roll(loads, 2 * horizon, 1)
    behind = pltpu.roll(pltpu.roll(loads, 2 * horizon - rest, 1), LOOPS, 0)
    block = jnp.where(lane < horizon, first, out[half:])
    return jnp.where(lane < 2 * horizon, block, jnp.where(row < LOOPS, ahead, behind))


def total_of(got_ref, horizon):
    total = jnp.sum(got_ref[...], axis=0)
    rest = LANES - 2 * horizon
    lane = iota(total.shape, 1)
    ahead = pltpu.roll(total, LANES - 2 * horizon, 1)
    behind = pltpu.roll(pltpu.roll(total, LANES - 2 * horizon + rest, 1), total.shape[0] - LOOPS, 0)
    return jnp.where(lane < rest, ahead, behind)


def near_of(got_ref, neighbors, per_floor, horizon, zones):
    half = zones // 2
    own = got_ref[pl.ds(lax.axis_index("floor") * per_floor, per_floor)].reshape(per_floor * half, LANES)
    column = iota((per_floor * half, zones), 0)
    low = (column // half) * zones + column % half
    count = neighbors.shape[0]
    pick_low = jnp.zeros(column.shape, jnp.float32)
    pick_high = pick_low
    for b in range(count):
        which = neighbors[b : b + 1]
        pick_low = pick_low + (which == low).astype(jnp.float32)
        pick_high = pick_high + (which == low + half).astype(jnp.float32)
    return (pltpu.roll(dot_rows(pick_low, own), horizon, 1) + dot_rows(pick_high, own)) / count


def widen(ref, scratch, shift):
    scratch[...] = jnp.zeros_like(scratch)
    scratch[: ref.shape[0], : ref.shape[1]] = ref[...]
    value = scratch[...]
    return pltpu.roll(value, shift, 1) if shift else value


def consensus(got_ref, out, price, multiplier, demand, neighbors, loop, per_floor, scale, horizon):
    zones = out.shape[0]
    lane = iota((zones, LANES), 1)
    excess = (total_of(got_ref, horizon) - demand) * scale
    shift = dot_rows(members(loop, price.shape[0]), excess + price)
    near = near_of(got_ref, neighbors, per_floor, horizon, zones)
    target = jnp.where(lane < horizon, out - shift, (out + near) / 2.0 - multiplier)
    return target, price + excess, multiplier + (out - near) / 2.0


def index_kernel(rows_ref):
    rows_ref[...] = iota(rows_ref.shape, 0)


def first_kernel(horizon, map_ref, plan_ref, loop_ref, rows_ref, out_ref, send_ref):
    zones, wide = map_ref.shape[0], map_ref.shape[1]
    out = outputs_of(lambda z: map_ref[z], plan_ref[...], zones, wide)
    out_ref[...] = out
    block = pack(out, loop_ref[...], rows_ref[...], horizon, zones)
    send_ref[...] = jnp.broadcast_to(block[None], send_ref.shape)


def middle_kernel(
    per_floor, scale, horizon,
    got_ref, out_ref, price_ref, mult_ref, demand_ref, nb_ref, loop_ref,
    offset_ref, factor_ref, map_ref,
    next_out_ref, next_price_ref, next_mult_ref, send_ref, wide8, wide16,
):
    zones, wide = map_ref.shape[0], map_ref.shape[1]
    target, price, mult = consensus(
        got_ref, out_ref[...], widen(price_ref, wide8, 0), widen(mult_ref, wide16, horizon),
        widen(demand_ref, wide8, 0), nb_ref[...], loop_ref[...], per_floor, scale, horizon,
    )
    next_price_ref[...] = price
    next_mult_ref[...] = mult
    control = decide(lambda z: factor_ref[z], target, zones, wide) - offset_ref[...]
    out = outputs_of(lambda z: map_ref[z], control, zones, wide)
    next_out_ref[...] = out
    block = pack(out, loop_ref[...], iota((zones // 2, LANES), 0), horizon, zones)
    send_ref[...] = jnp.broadcast_to(block[None], send_ref.shape)


def last_kernel(
    per_floor, scale, horizon,
    got_ref, out_ref, price_ref, mult_ref, demand_ref, nb_ref, loop_ref, offset_ref, factor_ref,
    control_ref, next_price_ref, next_mult_ref, wide8,
):
    zones, wide = factor_ref.shape[0], factor_ref.shape[1]
    target, price, mult = consensus(
        got_ref, out_ref[...], price_ref[...], mult_ref[...], widen(demand_ref, wide8, 0),
        nb_ref[...], loop_ref[...], per_floor, scale, horizon,
    )
    next_price_ref[...] = price[: next_price_ref.shape[0], :horizon]
    next_mult_ref[...] = pltpu.roll(mult, LANES - horizon, 1)[:, :horizon]
    control_ref[...] = decide(lambda z: factor_ref[z], target, zones, wide) - offset_ref[...]


def local(
    factor, plant_map, offset, start_plan, demand, start_price, start_multiplier, neighbors, loop_of_zone
):
    zones, wide, controls = plant_map.shape
    horizon = wide // 2
    half = zones // 2
    per_floor = lax.axis_size("zone")
    devices = lax.axis_size("floor") * per_floor
    scale = LOOPS / (zones * devices)
    loop_row = loop_of_zone[None, :]
    neighbors = neighbors.T
    vmem = pl.BlockSpec(memory_space=pltpu.VMEM)
    f32 = jnp.float32
    rows = jax.ShapeDtypeStruct((zones, LANES), f32)
    send = jax.ShapeDtypeStruct((devices, half, LANES), f32)
    eight = jax.ShapeDtypeStruct((half, LANES), f32)
    params = pltpu.CompilerParams(vmem_limit_bytes=24 * 1024 * 1024)

    row_index = pl.pallas_call(
        index_kernel,
        out_shape=jax.ShapeDtypeStruct((half, LANES), jnp.int32),
        out_specs=vmem,
        compiler_params=params,
        cost_estimate=pl.CostEstimate(
            flops=4000 * plant_map.size, bytes_accessed=80 * plant_map.size, transcendentals=0
        ),
        name="index",
    )()
    out, spread = pl.pallas_call(
        functools.partial(first_kernel, horizon),
        out_shape=(rows, send),
        in_specs=[vmem] * 4,
        out_specs=(vmem, vmem),
        compiler_params=params,
        name="first",
    )(plant_map, start_plan, loop_row, row_index)
    price, multiplier = start_price, start_multiplier
    for step in range(ITERS - 1):
        got = lax.all_to_all(spread, ("floor", "zone"), 0, 0)
        out, price, multiplier, spread = pl.pallas_call(
            functools.partial(middle_kernel, per_floor, scale, horizon),
            out_shape=(rows, eight, rows, send),
            in_specs=[vmem] * 10,
            out_specs=(vmem,) * 4,
            scratch_shapes=[pltpu.VMEM((half, LANES), f32), pltpu.VMEM((zones, LANES), f32)],
            compiler_params=params,
            name="middle",
        )(
            got, out, price, multiplier, demand, neighbors, loop_row,
            offset, factor, plant_map,
        )
    got = lax.all_to_all(spread, ("floor", "zone"), 0, 0)
    return pl.pallas_call(
        functools.partial(last_kernel, per_floor, scale, horizon),
        out_shape=(
            jax.ShapeDtypeStruct((zones, controls), f32),
            jax.ShapeDtypeStruct(start_price.shape, f32),
            jax.ShapeDtypeStruct(start_multiplier.shape, f32),
        ),
        in_specs=[vmem] * 9,
        out_specs=(vmem,) * 3,
        scratch_shapes=[pltpu.VMEM((half, LANES), f32)],
        compiler_params=params,
        name="last",
    )(got, out, price, multiplier, demand, neighbors, loop_row, offset, factor)


def solution(mesh):
    placed = (
        P(("floor", "zone"), None, None),
        P(("floor", "zone"), None, None),
        P(("floor", "zone"), None),
        P(("floor", "zone"), None),
        P(),
        P(),
        P(("floor", "zone"), None),
        P(("floor", "zone"), None),
        P(("floor", "zone")),
    )
    return jax.shard_map(
        local,
        mesh=mesh,
        in_specs=placed,
        out_specs=(P(("floor", "zone"), None), P(), P(("floor", "zone"), None)),
        check_vma=False,
    )
```
